128 devices in a mesh: bits: 128 (over y, z, x, core).
Axes of the slice: x: 4, y: 4, z: 4, core: 2. Of those that a mesh axis runs over, the one named last changes fastest.
Arguments:
- environment: float32 [2, 128, 64, 4096], P(None, 'bits'), may hold values from -6 to 6
- peps: float32 [2, 2, 8, 8, 8, 8], replicated, may hold values from -2 to 2
- operators: float32 [2, 2, 2], replicated, may hold values from -4 to 4
- gauge: float32 [128, 128], replicated, may hold values from -0.5 to 0.5
Outputs:
- absorbed: float32 [2, 128, 262144], P(None, None, 'bits')
- rms: float32 [2], replicated
The draws below stay inside these ranges and needn't reach their ends.
All inputs are finite; a program needn't handle non-finite values.
Results may differ from the reference program's by a relative error of at most 0.0003.
Values sent between devices are 32-bit elements; how exact they have to be, the bound alone decides.
No kernel may reach another device: no remote copies, remote signals or barrier semaphores. Data moves between devices by JAX's collectives and lax.ppermute only.
A program may use at most 512 MiB of HBM per device.

```python
import jax
import jax.numpy as jnp
from jax import lax

D = 8
PHYS = 2
CHI = 128
COLS = 2
NENV = 2
LEGS = 4096


def draw_peps(key, part):
    first, second = jax.random.split(jax.random.fold_in(key, 17), 2)
    shape = (COLS, PHYS, D, D, D, D)
    base = jax.random.truncated_normal(first, -4.0, 4.0, shape, jnp.float32)
    ramp = 3.0 ** (jnp.arange(D, dtype=jnp.float32) / (D - 1))
    rough = jnp.exp(jax.random.uniform(second, (COLS, 1, 1, 1, 1, D), jnp.float32, -0.2, 0.2))
    return (base / D * ramp * rough).astype(jnp.float32)


def levels(own_key, dims, shards, low, largest):
    loudness = 1.0
    for axis_at, parts in shards:
        draws = jax.random.uniform(jax.random.fold_in(jax.random.fold_in(own_key, 6), axis_at), (parts,), jnp.float32, low / len(shards), largest / len(shards))
        loudness = loudness * jnp.repeat(jnp.exp(draws), dims[axis_at] // parts).reshape((-1,) + (1,) * (len(dims) - 1 - axis_at))
    return loudness


def noise(stream_key, dims, spread, most, pieces=(), kind=jnp.bfloat16):
    entries = spread * jax.random.normal(stream_key, dims, jnp.float32)
    if pieces:
        entries = entries * levels(stream_key, dims, pieces, -0.22, 0.18)
    return jnp.clip(entries, -most, most).astype(kind)


def setup_inputs(seed: int = 0) -> dict:
    streams_of = jax.random.split(jax.random.key(seed), 5)
    environment = noise(streams_of[0], (NENV, CHI, D * D, LEGS), 1.0, 6.0, ((1, 128),), jnp.float32)
    peps = draw_peps(jax.random.fold_in(streams_of[4], 71), 0)
    operators = noise(streams_of[2], (COLS, PHYS, PHYS), 1.0, 4.0, (), jnp.float32)
    gauge = noise(streams_of[3], (CHI, CHI), CHI ** -0.5, 0.5, (), jnp.float32)
    return {"environment": environment, "peps": peps, "operators": operators, "gauge": gauge}


EPS = 1e-06

def absorb(state, peps, operators):
    count, rows = (state.shape[0], state.shape[1])
    width = peps.shape[2]
    columns = peps.shape[0]
    for column in range(columns):
        before = width ** (2 * column)
        after = width ** (2 * (columns - 1 - column))
        view = state.reshape(count, rows, width, width, before, width, width, after)
        bra_side = jnp.einsum('pq,qbvms->pbvms', operators[column], peps[column], precision=lax.Precision.HIGHEST)
        partial_value = jnp.einsum('eclbzuvx,plukr->ecrpbzkvx', view, peps[column], precision=lax.Precision.HIGHEST)
        state = jnp.einsum('ecrpbzkvx,pbvms->ecrszkmx', partial_value, bra_side, precision=lax.Precision.HIGHEST)
    return state.reshape(count, rows, -1)

def reference(environment, peps, operators, gauge):

    def single(block):
        grown = absorb(block[None], peps, operators)[0]
        return jnp.dot(gauge, grown, precision=lax.Precision.HIGHEST, preferred_element_type=jnp.float32)
    gauged = lax.map(single, environment)
    mean = lax.optimization_barrier(jnp.mean(gauged * gauged, axis=(1, 2)))
    absorbed = gauged * lax.rsqrt(mean + EPS)[:, None, None]
    return (absorbed, jnp.sqrt(mean))
```

```python
import functools
import jax, jax.numpy as jnp
from jax import lax
from jax.experimental import pallas as pl
from jax.experimental.pallas import tpu as pltpu

from jax.sharding import Mesh
from jax.sharding import PartitionSpec as P

BITS = ("bits_0", "bits_1", "bits_2", "bits_3")
EPS = 1e-06
F32, BF16 = jnp.float32, jnp.bfloat16
RS = 136
BS = 72
QS = 65
G = 4

def halves(x):
    hi = x.astype(BF16)
    return hi, (x - hi.astype(F32)).astype(BF16)

def wide(x):
    hi, lo = halves(x)
    return jnp.concatenate([hi, hi, lo], axis=1)

def tall(x):
    hi, lo = halves(x)
    return jnp.concatenate([hi, lo, hi], axis=0)

def mm(w, x):
    return jnp.dot(w, tall(x), preferred_element_type=F32)

def absorb_kernel(env, p, ops, out, x_s, t_s, s_s, bra_w, ket_w):
    lane = lax.broadcasted_iota(jnp.int32, (8, 128), 1)
    low = lane < 64
    for j in range(2):
        pj = p[128 * j:128 * (j + 1), :]
        ket_w[j] = wide(pj.T)
        for a in range(2):
            q = ops[j, a, 0] * pj[:64] + ops[j, a, 1] * pj[64:]
            if j == 0:
                q = jnp.swapaxes(q.reshape(8, 8, 64), 0, 1).reshape(64, 64)
            bra_w[j, 64 * a:64 * (a + 1), :] = wide(q.T)

    def load(kl, _):
        for c in range(32):
            rows = pl.ds(pl.multiple_of(8 * kl, 8), 8)
            v0 = env[0, 0, rows, 128 * c:128 * (c + 1)]
            v1 = env[1, 0, rows, 128 * c:128 * (c + 1)]
            k0, bh = c // 4, c % 4
            at = pl.multiple_of((kl * 8 + k0) * 64 + bh * 16, 16)
            r0 = pltpu.roll(v0, 64, 1)
            r1 = pltpu.roll(v1, 64, 1)
            x_s[pl.ds(at, 8), :] = jnp.where(low, v0, r1)
            x_s[pl.ds(at + 8, 8), :] = jnp.where(low, r0, v1)
        return 0
    lax.fori_loop(0, 8, load, 0)

    def bra(j):
        w = bra_w[j]
        def step(i, _):
            x = jnp.concatenate([x_s[pl.ds(pl.multiple_of((i * G + g) * 64, 64), 64), :] for g in range(G)], axis=1)
            y = mm(w, x)
            for g in range(G):
                for a in range(2):
                    t_s[pl.ds(a * 64 + i * G + g, 64, stride=RS), :] = y[64 * a:64 * (a + 1), 128 * g:128 * (g + 1)]
            return 0
        lax.fori_loop(0, 64 // G, step, 0)

    def ket(j, put):
        w = ket_w[j]
        def step(i, _):
            x = jnp.concatenate([t_s[pl.ds(pl.multiple_of((i * G + g) * RS, 8), 128), :] for g in range(G)], axis=1)
            y = mm(w, x)
            for g in range(G):
                put(i * G + g, y[:, 128 * g:128 * (g + 1)])
            return 0
        lax.fori_loop(0, 64 // G, step, 0)

    bra(0)

    def put0(b, y):
        bd, br = b // 8, b % 8
        for kd in range(8):
            s_s[pl.ds(br * 8 * BS + (bd % 2) * 32 + kd * 4 + bd // 2, 8, stride=BS), :] = y[8 * kd:8 * (kd + 1)]
    ket(0, put0)

    def turn(i, _):
        br, kr = i // 8, i % 8
        z = s_s[pl.ds(pl.multiple_of(i * BS, 8), 64), :].T
        z = jnp.concatenate([z[:64], z[64:]], axis=1)
        for k1 in range(8):
            x_s[pl.ds(pl.multiple_of((kr * 8 + k1) * 64 + br * 8, 8), 8), :] = z[8 * k1:8 * (k1 + 1)]
        return 0
    lax.fori_loop(0, 64, turn, 0)

    bra(1)

    def put1(b, y):
        bd, br = b // 8, b % 8
        for kd in range(8):
            s_s[pl.ds(br * BS + kd * 8 + bd, 8, stride=8 * BS), :] = y[8 * kd:8 * (kd + 1)]
    ket(1, put1)

    def leave(i, _):
        z = s_s[pl.ds(pl.multiple_of(i * BS, 8), 64), :].T
        for e in range(2):
            z_e = jnp.concatenate([z[64 * e:64 * e + 32], z[64 * e + 32:64 * e + 64]], axis=1)
            for h in range(2):
                out[2 * i + h, 16 * e:16 * (e + 1), :] = z_e[16 * h:16 * (h + 1)]
        return 0
    lax.fori_loop(0, 64, leave, 0)

def absorb(env, p, ops):
    vm = pl.BlockSpec(memory_space=pltpu.VMEM)
    return pl.pallas_call(
        absorb_kernel,
        out_shape=jax.ShapeDtypeStruct((128, 32, 128), F32),
        in_specs=[vm, vm, pl.BlockSpec(memory_space=pltpu.SMEM)],
        out_specs=vm,
        scratch_shapes=[
            pltpu.VMEM((4096, 128), F32),
            pltpu.VMEM((64 * RS, 128), F32),
            pltpu.VMEM((64 * BS, 128), F32),
            pltpu.VMEM((2, 128, 192), BF16),
            pltpu.VMEM((2, 64, 384), BF16),
        ],
        compiler_params=pltpu.CompilerParams(vmem_limit_bytes=40 << 20),
        cost_estimate=pl.CostEstimate(flops=2 << 30, bytes_accessed=4 << 20, transcendentals=0),
        name="absorb",
    )(env, p, ops)

def gauge_kernel(r, gm, out, sq, w_s):
    w_s[...] = wide(gm[...])
    lane = lax.broadcasted_iota(jnp.int32, (1, 128), 1)
    row = jnp.zeros((1, 128), F32)
    w = w_s[...]
    for e in range(2):
        tot = jnp.zeros((8, 128), F32)
        for b in range(0, 16, G):
            x = jnp.concatenate([r[pl.ds(e * 16 + b + g, 128, stride=32), :] for g in range(G)], axis=1)
            y = mm(w, x)
            out[e, :, 128 * b:128 * (b + G)] = y
            q = y * y
            q = q.reshape(16, 8, 128 * G).sum(0)
            for g in range(G):
                tot = tot + q[:, 128 * g:128 * (g + 1)]
        row = jnp.where(lane == e, jnp.sum(tot), row)
    sq[...] = jnp.broadcast_to(row[None], (128, 1, 128))

def gauge(r, gm):
    vm = pl.BlockSpec(memory_space=pltpu.VMEM)
    return pl.pallas_call(
        gauge_kernel,
        out_shape=(jax.ShapeDtypeStruct((2, 128, 2048), F32), jax.ShapeDtypeStruct((128, 1, 128), F32)),
        in_specs=[vm, vm],
        out_specs=(vm, vm),
        scratch_shapes=[pltpu.VMEM((128, 384), BF16)],
        compiler_params=pltpu.CompilerParams(vmem_limit_bytes=40 << 20),
        cost_estimate=pl.CostEstimate(flops=1 << 29, bytes_accessed=4 << 20, transcendentals=0),
        name="gauge",
    )(r.reshape(4096, 128), gm)

def scale_kernel(entries, x, sums, out, rms):
    total = jnp.sum(sums[...], axis=(0, 1)).reshape(1, 128)
    lane = lax.broadcasted_iota(jnp.int32, (1, 128), 1)
    for e in range(2):
        mean = jnp.sum(jnp.where(lane == e, total, 0.0), axis=1, keepdims=True) / entries
        at = pl.ds(pl.multiple_of(pl.program_id(0) * 16, 16), 16)
        out[e] = x[e, at, :] * lax.rsqrt(mean + EPS)
        @pl.when(pl.program_id(0) == 0)
        def _():
            rms[e] = jnp.sqrt(mean)[0, 0]

def scale(x, sums, entries):
    vm = pl.BlockSpec(memory_space=pltpu.VMEM)
    return pl.pallas_call(
        functools.partial(scale_kernel, entries),
        grid=(8,),
        out_shape=(jax.ShapeDtypeStruct((2, 128, 2048), F32), jax.ShapeDtypeStruct((2,), F32)),
        in_specs=[vm, vm],
        out_specs=(pl.BlockSpec((2, 16, 2048), lambda i: (0, i, 0)), pl.BlockSpec(memory_space=pltpu.SMEM)),
        compiler_params=pltpu.CompilerParams(vmem_limit_bytes=40 << 20),
        cost_estimate=pl.CostEstimate(flops=1 << 19, bytes_accessed=4 << 20, transcendentals=0),
        name="scale",
    )(x, sums)

def body(environment, peps, operators, gauge_matrix):
    blocks = absorb(environment, peps.reshape(256, 64), operators)
    merged = lax.all_to_all(blocks, BITS, 0, 0, tiled=True)
    gauged, sums = gauge(merged, gauge_matrix)
    sums = lax.all_to_all(sums, BITS, 0, 0, tiled=True)
    entries = gauged.shape[1] * gauged.shape[2] * lax.axis_size(BITS)
    return scale(gauged, sums, entries)


def solution(mesh):
    torus = Mesh(mesh.devices.reshape(4, 4, 4, 2), BITS)
    in_specs = (P(None, BITS, None, None), P(), P(), P())
    out_specs = (P(None, None, BITS), P())
    return jax.shard_map(body, mesh=torus, in_specs=in_specs, out_specs=out_specs, check_vma=False)
```

```python
import functools
import jax, jax.numpy as jnp
from jax import lax
from jax.experimental import pallas as pl
from jax.experimental.pallas import tpu as pltpu

from jax.sharding import Mesh
from jax.sharding import PartitionSpec as P

BITS = ("bits_0", "bits_1", "bits_2", "bits_3")
EPS = 1e-06
F32, BF16 = jnp.float32, jnp.bfloat16
UB = 4
UK = 4
UT = 8
RS = 132
BS = 68
G = 4


def halves(x):
    hi = x.astype(BF16)
    return hi, (x - hi.astype(F32)).astype(BF16)


def wide(x):
    hi, lo = halves(x)
    return jnp.concatenate([hi, hi, lo], axis=1)


def tall(x):
    hi, lo = halves(x)
    return jnp.concatenate([hi, lo, hi], axis=0)


def mm(w, x):
    return jnp.dot(w, tall(x), preferred_element_type=F32)


def loop(count, unroll, step):
    def several(i, carry):
        for u in range(unroll):
            step(i * unroll + u)
        return carry

    lax.fori_loop(0, count // unroll, several, 0)


def swap(a, b, low):
    return jnp.where(low, a, pltpu.roll(b, 64, 1)), jnp.where(low, pltpu.roll(a, 64, 1), b)


def absorb_kernel(env, p, ops, out, x_s, t_s, s_s, bra_w, ket_w):
    low = lax.broadcasted_iota(jnp.int32, (8, 128), 1) < 64
    for j in range(2):
        pj = p[128 * j : 128 * (j + 1), :]
        ket_w[j] = wide(pj.T)
        for a in range(2):
            q = ops[j, a, 0] * pj[:64] + ops[j, a, 1] * pj[64:]
            if j == 0:
                q = jnp.swapaxes(q.reshape(8, 8, 64), 0, 1).reshape(64, 64)
            bra_w[j, 64 * a : 64 * (a + 1), :] = wide(q.T)

    def first(at):
        kl, k0 = at // 8, at % 8
        rows = pl.ds(pl.multiple_of(8 * kl, 8), 8)
        pieces = []
        for c in range(4):
            lanes = pl.ds(pl.multiple_of(k0 * 512 + 128 * c, 128), 128)
            pieces += swap(env[0, 0, rows, lanes], env[1, 0, rows, lanes], low)
        return jnp.concatenate(pieces, axis=0)

    def second(at):
        return x_s[pl.ds(pl.multiple_of(at * 64, 64), 64), :]

    def bra(j, get):
        def step(i):
            y = mm(bra_w[j], jnp.concatenate([get(i * G + g) for g in range(G)], axis=1))
            for g in range(G):
                for a in range(2):
                    t_s[pl.ds(a * 64 + i * G + g, 64, stride=RS), :] = y[64 * a : 64 * (a + 1), 128 * g : 128 * (g + 1)]

        loop(64 // G, UB, step)

    def ket(j, put):
        def step(i):
            x = jnp.concatenate([t_s[pl.ds((i * G + g) * RS, 128), :] for g in range(G)], axis=1)
            y = mm(ket_w[j], x)
            for g in range(G):
                put(i * G + g, y[:, 128 * g : 128 * (g + 1)])

        loop(64 // G, UK, step)

    bra(0, first)

    def put0(b, y):
        bd, br = b // 8, b % 8
        for kd in range(8):
            s_s[pl.ds(br * 8 * BS + (bd % 2) * 32 + kd * 4 + bd // 2, 8, stride=BS), :] = y[8 * kd : 8 * (kd + 1)]

    ket(0, put0)

    def turned(i):
        return jnp.concatenate([s_s[pl.ds(2 * i * BS, 64), :], s_s[pl.ds((2 * i + 1) * BS, 64), :]], axis=0).T

    def turn(i):
        br, kr = i // 4, 2 * (i % 4)
        z = turned(i)
        for k1 in range(8):
            z0, z1 = swap(z[8 * k1 : 8 * k1 + 8], z[64 + 8 * k1 : 64 + 8 * k1 + 8], low)
            x_s[pl.ds(pl.multiple_of((kr * 8 + k1) * 64 + br * 8, 8), 8), :] = z0
            x_s[pl.ds(pl.multiple_of((kr * 8 + 8 + k1) * 64 + br * 8, 8), 8), :] = z1

    loop(32, UT, turn)
    bra(1, second)

    def put1(b, y):
        bd, br = b // 8, b % 8
        for kd in range(8):
            s_s[pl.ds(kd * 8 + bd + br * 8 * BS, 8, stride=BS), :] = y[8 * kd : 8 * (kd + 1)]

    ket(1, put1)

    def leave(i):
        br, kr = i // 4, 2 * (i % 4)
        z = turned(i)
        for e in range(2):
            for r in range(4):
                z0, z1 = swap(z[64 * e + 8 * r : 64 * e + 8 * r + 8], z[64 * e + 32 + 8 * r : 64 * e + 40 + 8 * r], low)
                h, row = r // 2, 16 * e + 8 * (r % 2)
                out[2 * (kr * 8 + br) + h, row : row + 8, :] = z0
                out[2 * (kr * 8 + 8 + br) + h, row : row + 8, :] = z1

    loop(32, UT, leave)


def absorb(env, p, ops):
    vm = pl.BlockSpec(memory_space=pltpu.VMEM)
    return pl.pallas_call(
        absorb_kernel,
        out_shape=jax.ShapeDtypeStruct((128, 32, 128), F32),
        in_specs=[vm, vm, pl.BlockSpec(memory_space=pltpu.SMEM)],
        out_specs=vm,
        scratch_shapes=[
            pltpu.VMEM((4096, 128), F32),
            pltpu.VMEM((64 * RS, 128), F32),
            pltpu.VMEM((64 * BS, 128), F32),
            pltpu.VMEM((2, 128, 192), BF16),
            pltpu.VMEM((2, 64, 384), BF16),
        ],
        compiler_params=pltpu.CompilerParams(vmem_limit_bytes=40 << 20),
        cost_estimate=pl.CostEstimate(flops=2 << 30, bytes_accessed=4 << 20, transcendentals=0),
        name="absorb",
    )(env, p, ops)

def gauge_kernel(r, gm, out, sq, w_s):
    w_s[...] = wide(gm[...])
    lane = lax.broadcasted_iota(jnp.int32, (1, 128), 1)
    row = jnp.zeros((1, 128), F32)
    w = w_s[...]
    for e in range(2):
        tot = jnp.zeros((8, 128), F32)
        for b in range(0, 16, G):
            x = jnp.concatenate([r[pl.ds(e * 16 + b + g, 128, stride=32), :] for g in range(G)], axis=1)
            y = mm(w, x)
            out[e, :, 128 * b:128 * (b + G)] = y
            q = y * y
            q = q.reshape(16, 8, 128 * G).sum(0)
            for g in range(G):
                tot = tot + q[:, 128 * g:128 * (g + 1)]
        row = jnp.where(lane == e, jnp.sum(tot), row)
    sq[...] = jnp.broadcast_to(row[None], (128, 1, 128))

def gauge(r, gm):
    vm = pl.BlockSpec(memory_space=pltpu.VMEM)
    return pl.pallas_call(
        gauge_kernel,
        out_shape=(jax.ShapeDtypeStruct((2, 128, 2048), F32), jax.ShapeDtypeStruct((128, 1, 128), F32)),
        in_specs=[vm, vm],
        out_specs=(vm, vm),
        scratch_shapes=[pltpu.VMEM((128, 384), BF16)],
        compiler_params=pltpu.CompilerParams(vmem_limit_bytes=40 << 20),
        cost_estimate=pl.CostEstimate(flops=1 << 29, bytes_accessed=4 << 20, transcendentals=0),
        name="gauge",
    )(r.reshape(4096, 128), gm)

def scale_kernel(entries, x, sums, out, rms):
    total = jnp.sum(sums[...], axis=(0, 1)).reshape(1, 128)
    lane = lax.broadcasted_iota(jnp.int32, (1, 128), 1)
    for e in range(2):
        mean = jnp.sum(jnp.where(lane == e, total, 0.0), axis=1, keepdims=True) / entries
        at = pl.ds(pl.multiple_of(pl.program_id(0) * 16, 16), 16)
        out[e] = x[e, at, :] * lax.rsqrt(mean + EPS)
        @pl.when(pl.program_id(0) == 0)
        def _():
            rms[e] = jnp.sqrt(mean)[0, 0]

def scale(x, sums, entries):
    vm = pl.BlockSpec(memory_space=pltpu.VMEM)
    return pl.pallas_call(
        functools.partial(scale_kernel, entries),
        grid=(8,),
        out_shape=(jax.ShapeDtypeStruct((2, 128, 2048), F32), jax.ShapeDtypeStruct((2,), F32)),
        in_specs=[vm, vm],
        out_specs=(pl.BlockSpec((2, 16, 2048), lambda i: (0, i, 0)), pl.BlockSpec(memory_space=pltpu.SMEM)),
        compiler_params=pltpu.CompilerParams(vmem_limit_bytes=40 << 20),
        cost_estimate=pl.CostEstimate(flops=1 << 19, bytes_accessed=4 << 20, transcendentals=0),
        name="scale",
    )(x, sums)

def body(environment, peps, operators, gauge_matrix):
    blocks = absorb(environment, peps.reshape(256, 64), operators)
    merged = lax.all_to_all(blocks, BITS, 0, 0, tiled=True)
    gauged, sums = gauge(merged, gauge_matrix)
    sums = lax.all_to_all(sums, BITS, 0, 0, tiled=True)
    entries = gauged.shape[1] * gauged.shape[2] * lax.axis_size(BITS)
    return scale(gauged, sums, entries)


def solution(mesh):
    torus = Mesh(mesh.devices.reshape(4, 4, 4, 2), BITS)
    in_specs = (P(None, BITS, None, None), P(), P(), P())
    out_specs = (P(None, None, BITS), P())
    return jax.shard_map(body, mesh=torus, in_specs=in_specs, out_specs=out_specs, check_vma=False)
```

```python
import functools

import jax
import jax.numpy as jnp
from jax import lax
from jax.experimental import pallas as pl
from jax.experimental.pallas import tpu as pltpu
from jax.sharding import Mesh
from jax.sharding import PartitionSpec as P

BITS = ("bits_0", "bits_1", "bits_2", "bits_3")
EPS = 1e-06
F32, BF16 = jnp.float32, jnp.bfloat16
RS = 132
BS = 68
G = 4
UB0 = 4
UB = 8
UK = 8
UT = 32


def halves(x):
    hi = x.astype(BF16)
    return hi, (x - hi.astype(F32)).astype(BF16)


def tall(x):
    hi, lo = halves(x)
    return jnp.concatenate([hi, lo, hi], axis=0)


def mm(w, x):
    return jnp.dot(w, tall(x), preferred_element_type=F32)


def loop(count, unroll, step):
    def several(i, carry):
        for u in range(unroll):
            step(i * unroll + u)
        return carry

    if unroll == count:
        several(0, 0)
    else:
        lax.fori_loop(0, count // unroll, several, 0)


def rows_at(at, size):
    return pl.ds(at if isinstance(at, int) else pl.multiple_of(at, 8), size)


def swap(a, b, low):
    return jnp.where(low, a, pltpu.roll(b, 64, 1)), jnp.where(low, pltpu.roll(a, 64, 1), b)


def absorb_kernel(env, p, ops, out, env_s, p_s, ops_s, x_s, t_s, s_s, bra_w, ket_w, env_sem, p_sem, ops_sem):
    small = [pltpu.make_async_copy(p, p_s, p_sem), pltpu.make_async_copy(ops, ops_s, ops_sem)]
    for copy in small:
        copy.start()

    def chunk(kl):
        rows = pl.ds(8 * kl, 8)
        return pltpu.make_async_copy(env.at[:, :, rows, :], env_s.at[:, :, rows, :], env_sem.at[kl])

    for kl in range(8):
        chunk(kl).start()
    low = lax.broadcasted_iota(jnp.int32, (8, 128), 1) < 64
    for copy in small:
        copy.wait()
    turned_p = jnp.swapaxes(p_s[...], 0, 1)
    w = jnp.concatenate([turned_p[d].T for d in range(8)], axis=0)
    row = lax.broadcasted_iota(jnp.int32, (64, 64), 0)
    col = lax.broadcasted_iota(jnp.int32, (64, 64), 1)
    exchange = jnp.where(row == (col % 8) * 8 + col // 8, 1.0, 0.0).astype(BF16)
    for j in range(2):
        wj = w[:, 128 * j : 128 * (j + 1)]
        hi, lo = halves(wj)
        ket_w[j] = jnp.concatenate([hi, hi, lo], axis=1)
        for a in range(2):
            parts = halves(ops_s[j, a, 0] * wj[:, :64] + ops_s[j, a, 1] * wj[:, 64:])
            if j == 0:
                parts = [jnp.dot(part, exchange, preferred_element_type=F32).astype(BF16) for part in parts]
            hi, lo = parts
            bra_w[j, 64 * a : 64 * (a + 1), :] = jnp.concatenate([hi, hi, lo], axis=1)

    def first(kl, k0):
        rows = rows_at(8 * kl, 8)
        pieces = []
        for c in range(4):
            lanes = pl.ds(k0 * 512 + 128 * c, 128)
            pieces += swap(env_s[0, 0, rows, lanes], env_s[1, 0, rows, lanes], low)
        return jnp.concatenate(pieces, axis=0)

    def second(at):
        return x_s[rows_at(at * 64, 64), :]

    def bra_group(j, at, xs):
        y = mm(bra_w[j], jnp.concatenate(xs, axis=1))
        for g in range(G):
            for a in range(2):
                t_s[pl.ds(a * 64 + at + g, 64, stride=RS), :] = y[64 * a : 64 * (a + 1), 128 * g : 128 * (g + 1)]

    def first_group(i):
        for kl_off in range(2):
            chunk(2 * i + kl_off).wait()
        for kl_off in range(2):
            kl = 2 * i + kl_off
            for k0 in range(0, 8, G):
                bra_group(0, kl * 8 + k0, [first(kl, k0 + g) for g in range(G)])

    loop(4, UB0 // 4, first_group)

    def ket(j, put):
        def step(i):
            x = jnp.concatenate([t_s[pl.ds((i * G + g) * RS, 128), :] for g in range(G)], axis=1)
            y = mm(ket_w[j], x)
            for g in range(G):
                put(i * G + g, y[:, 128 * g : 128 * (g + 1)])

        loop(64 // G, UK, step)

    def put0(b, y):
        bd, br = b // 8, b % 8
        for kd in range(8):
            s_s[pl.ds(br * 8 * BS + (bd % 2) * 32 + kd * 4 + bd // 2, 8, stride=BS), :] = y[8 * kd : 8 * (kd + 1)]

    ket(0, put0)

    def turned(i):
        return jnp.concatenate([s_s[pl.ds(2 * i * BS, 64), :], s_s[pl.ds((2 * i + 1) * BS, 64), :]], axis=0).T

    def turn(i):
        br, kr = i // 4, 2 * (i % 4)
        z = turned(i)
        for k1 in range(8):
            z0, z1 = swap(z[8 * k1 : 8 * k1 + 8], z[64 + 8 * k1 : 64 + 8 * k1 + 8], low)
            x_s[rows_at((kr * 8 + k1) * 64 + br * 8, 8), :] = z0
            x_s[rows_at((kr * 8 + 8 + k1) * 64 + br * 8, 8), :] = z1

    loop(32, UT, turn)
    loop(64 // G, UB, lambda i: bra_group(1, i * G, [second(i * G + g) for g in range(G)]))

    def put1(b, y):
        bd, br = b // 8, b % 8
        for kd in range(8):
            s_s[pl.ds(kd * 8 + bd + br * 8 * BS, 8, stride=BS), :] = y[8 * kd : 8 * (kd + 1)]

    ket(1, put1)

    def leave(i):
        br, kr = i // 4, 2 * (i % 4)
        z = turned(i)
        for e in range(2):
            for r in range(4):
                z0, z1 = swap(z[64 * e + 8 * r : 64 * e + 8 * r + 8], z[64 * e + 32 + 8 * r : 64 * e + 40 + 8 * r], low)
                h, row = r // 2, 16 * e + 8 * (r % 2)
                out[2 * (kr * 8 + br) + h, row : row + 8, :] = z0
                out[2 * (kr * 8 + 8 + br) + h, row : row + 8, :] = z1

    loop(32, UT, leave)


HBM = pl.BlockSpec(memory_space=pltpu.HBM)
VMEM = pl.BlockSpec(memory_space=pltpu.VMEM)


def absorb(env, p, ops):
    return pl.pallas_call(
        absorb_kernel,
        out_shape=jax.ShapeDtypeStruct((128, 32, 128), F32),
        in_specs=[HBM, HBM, HBM],
        out_specs=VMEM,
        scratch_shapes=[
            pltpu.VMEM((2, 1, 64, 4096), F32),
            pltpu.VMEM((256, 8, 8), F32),
            pltpu.SMEM((2, 2, 2), F32),
            pltpu.VMEM((4096, 128), F32),
            pltpu.VMEM((64 * RS, 128), F32),
            pltpu.VMEM((64 * BS, 128), F32),
            pltpu.VMEM((2, 128, 192), BF16),
            pltpu.VMEM((2, 64, 384), BF16),
            pltpu.SemaphoreType.DMA((8,)),
            pltpu.SemaphoreType.DMA,
            pltpu.SemaphoreType.DMA,
        ],
        compiler_params=pltpu.CompilerParams(vmem_limit_bytes=40 << 20),
        cost_estimate=pl.CostEstimate(flops=2 << 30, bytes_accessed=4 << 20, transcendentals=0),
        name="absorb",
    )(env, p, ops)


def absorb_raw(env, peps, ops):
    return absorb(*[pltpu.with_memory_space_constraint(v, pltpu.HBM) for v in (env, peps.reshape(256, 8, 8), ops)])


def gauge_kernel(r, gm, out, sq, w_s):
    hi, lo = halves(gm[...])
    w_s[...] = jnp.concatenate([hi, hi, lo], axis=1)
    lane = lax.broadcasted_iota(jnp.int32, (1, 128), 1)
    row = jnp.zeros((1, 128), F32)
    w = w_s[...]
    for e in range(2):
        tot = jnp.zeros((8, 128), F32)
        for b in range(0, 16, 4):
            x = jnp.concatenate([r[pl.ds(e * 16 + b + g, 128, stride=32), :] for g in range(4)], axis=1)
            y = mm(w, x)
            out[e, :, 128 * b : 128 * (b + 4)] = y
            q = (y * y).reshape(16, 8, 512).sum(0)
            for g in range(4):
                tot = tot + q[:, 128 * g : 128 * (g + 1)]
        row = jnp.where(lane == e, jnp.sum(tot), row)
    sq[...] = jnp.broadcast_to(row[None], (128, 1, 128))


def gauge(r, gm):
    return pl.pallas_call(
        gauge_kernel,
        out_shape=(jax.ShapeDtypeStruct((2, 128, 2048), F32), jax.ShapeDtypeStruct((128, 1, 128), F32)),
        in_specs=[VMEM, VMEM],
        out_specs=(VMEM, VMEM),
        scratch_shapes=[pltpu.VMEM((128, 384), BF16)],
        compiler_params=pltpu.CompilerParams(vmem_limit_bytes=40 << 20),
        cost_estimate=pl.CostEstimate(flops=1 << 29, bytes_accessed=4 << 20, transcendentals=0),
        name="gauge",
    )(r.reshape(4096, 128), gm)


def scale_kernel(entries, x, sums, out, rms, y_s, sems):
    total = jnp.sum(sums[...], axis=0)
    lane = lax.broadcasted_iota(jnp.int32, (1, 128), 1)
    copies = []
    for e in range(2):
        mean = jnp.sum(jnp.where(lane == e, total, 0.0), axis=1, keepdims=True) / entries
        factor = lax.rsqrt(mean + EPS)
        for c in range(8):
            at = pl.ds(16 * c, 16)
            y_s[e, at, :] = x[e, at, :] * factor
            copy = pltpu.make_async_copy(y_s.at[e, at, :], out.at[e, at, :], sems.at[8 * e + c])
            copy.start()
            copies.append(copy)
        rms[e] = jnp.sqrt(mean)[0, 0]
    for copy in copies:
        copy.wait()


def scale(x, sums, entries):
    return pl.pallas_call(
        functools.partial(scale_kernel, entries),
        out_shape=(jax.ShapeDtypeStruct((2, 128, 2048), F32), jax.ShapeDtypeStruct((2,), F32)),
        in_specs=[VMEM, VMEM],
        out_specs=(HBM, pl.BlockSpec(memory_space=pltpu.SMEM)),
        scratch_shapes=[pltpu.VMEM((2, 128, 2048), F32), pltpu.SemaphoreType.DMA((16,))],
        compiler_params=pltpu.CompilerParams(vmem_limit_bytes=40 << 20),
        cost_estimate=pl.CostEstimate(flops=1 << 19, bytes_accessed=4 << 20, transcendentals=0),
        name="scale",
    )(x, sums)


def body(environment, peps, operators, gauge_matrix):
    blocks = absorb_raw(environment, peps, operators)
    merged = lax.all_to_all(blocks, BITS, 0, 0, tiled=True)
    gauged, sums = gauge(merged, gauge_matrix)
    sums = lax.all_to_all(sums, BITS, 0, 0, tiled=True)
    entries = gauged.shape[1] * gauged.shape[2] * lax.axis_size(BITS)
    return scale(gauged, sums, entries)


def solution(mesh):
    torus = Mesh(mesh.devices.reshape(4, 4, 4, 2), BITS)
    in_specs = (P(None, BITS, None, None), P(), P(), P())
    out_specs = (P(None, None, BITS), P())
    return jax.shard_map(body, mesh=torus, in_specs=in_specs, out_specs=out_specs, check_vma=False)
```

```python
import functools

import jax
import jax.numpy as jnp
from jax import lax
from jax.experimental import pallas as pl
from jax.experimental.pallas import tpu as pltpu
from jax.sharding import Mesh
from jax.sharding import PartitionSpec as P

BITS = ("bits_0", "bits_1", "bits_2", "bits_3")
EPS = 1e-06
F32, BF16 = jnp.float32, jnp.bfloat16
RS = 132
BS = 68
G = 4
W0 = 8
UB = 16
UBR = 8
KM = 1


def halves(x):
    hi = x.astype(BF16)
    return hi, (x - hi.astype(F32)).astype(BF16)


def tall(x):
    hi, lo = halves(x)
    return jnp.concatenate([hi, lo, hi], axis=0)


def mm(w, x):
    return jnp.dot(w, tall(x), preferred_element_type=F32)


def loop(count, unroll, step):
    def several(i, carry):
        for u in range(unroll):
            step(i * unroll + u)
        return carry

    if unroll == count:
        several(0, 0)
    else:
        lax.fori_loop(0, count // unroll, several, 0)


def rows_at(at, size):
    return pl.ds(at if isinstance(at, int) else pl.multiple_of(at, 8), size)


def swap(a, b, low):
    return jnp.where(low, a, pltpu.roll(b, 64, 1)), jnp.where(low, pltpu.roll(a, 64, 1), b)


def absorb_kernel(env, p, ops, out, env_s, p_s, q_s, ops_s, x_s, t_s, s_s, bra_w, ket_w, env_sem, p_sem, ops_sem):
    small = [pltpu.make_async_copy(p, p_s, p_sem), pltpu.make_async_copy(ops, ops_s, ops_sem)]
    for copy in small:
        copy.start()

    def chunk(kl):
        rows = pl.ds(8 * kl, 8)
        return pltpu.make_async_copy(env.at[:, :, rows, :], env_s.at[:, :, rows, :], env_sem.at[kl])

    for kl in range(8):
        chunk(kl).start()
    low = lax.broadcasted_iota(jnp.int32, (8, 128), 1) < 64
    for copy in small:
        copy.wait()
    for g in range(32):
        q_s[:, 8 * g : 8 * g + 8, :] = jnp.swapaxes(p_s[8 * g : 8 * g + 8], 0, 1)
    row = lax.broadcasted_iota(jnp.int32, (64, 64), 0)
    col = lax.broadcasted_iota(jnp.int32, (64, 64), 1)
    exchange = jnp.where(row == (col % 8) * 8 + col // 8, 1.0, 0.0).astype(BF16)
    for j in range(2):
        wj = jnp.concatenate([q_s[d, 128 * j : 128 * (j + 1), :].T for d in range(8)], axis=0)
        hi, lo = halves(wj)
        ket_w[j, :64] = jnp.concatenate([hi, hi], axis=1)
        ket_w[j, 64:] = jnp.concatenate([lo, jnp.zeros_like(lo)], axis=1)
        for a in range(2):
            parts = halves(ops_s[j, a, 0] * wj[:, :64] + ops_s[j, a, 1] * wj[:, 64:])
            if j == 0:
                parts = [jnp.dot(part, exchange, preferred_element_type=F32).astype(BF16) for part in parts]
            hi, lo = parts
            bra_w[j, 64 * a : 64 * (a + 1), :] = jnp.concatenate([hi, hi, lo], axis=1)

    def first(kl, k0):
        rows = rows_at(8 * kl, 8)
        pieces = []
        for c in range(4):
            lanes = pl.ds(k0 * 512 + 128 * c, 128)
            pieces += swap(env_s[0, 0, rows, lanes], env_s[1, 0, rows, lanes], low)
        return jnp.concatenate(pieces, axis=0)

    def second(at):
        return x_s[rows_at(at * 64, 64), :]

    def bra_group(j, at, xs):
        y = mm(bra_w[j], jnp.concatenate(xs, axis=1))
        for g in range(G):
            for a in range(2):
                t_s[pl.ds(a * 64 + at + g, 64, stride=RS), :] = y[64 * a : 64 * (a + 1), 128 * g : 128 * (g + 1)]

    for start in range(0, 8, W0):
        for kl in range(start, start + W0):
            chunk(kl).wait()
        for kl in range(start, start + W0):
            for k0 in range(0, 8, G):
                bra_group(0, kl * 8 + k0, [first(kl, k0 + g) for g in range(G)])

    def ket(j, br, put):
        for start in range(0, 8, G):
            x = jnp.concatenate([t_s[pl.ds(((start + g) * 8 + br) * RS, 128), :] for g in range(G)], axis=1)
            x = jnp.concatenate(halves(x), axis=0)
            if KM:
                y = jnp.dot(ket_w[j], x, preferred_element_type=F32)
                y = y[:64] + y[64:]
            else:
                y = jnp.dot(ket_w[j, :64], x, preferred_element_type=F32) + jnp.dot(ket_w[j, 64:], x, preferred_element_type=F32)
            for g in range(G):
                put((start + g) * 8 + br, y[:, 128 * g : 128 * (g + 1)])

    def put0(b, y):
        bd, br = b // 8, b % 8
        for kd in range(8):
            s_s[pl.ds(br * 8 * BS + (bd % 2) * 32 + kd * 4 + bd // 2, 8, stride=BS), :] = y[8 * kd : 8 * (kd + 1)]

    def turned(i):
        return jnp.concatenate([s_s[pl.ds(2 * i * BS, 64), :], s_s[pl.ds((2 * i + 1) * BS, 64), :]], axis=0).T

    def sweep(j, put, finish):
        def step(br):
            ket(j, br, put)
            for i in range(4):
                finish(br * 4 + i)

        loop(8, UBR, step)

    def turn(i):
        br, kr = i // 4, 2 * (i % 4)
        z = turned(i)
        for k1 in range(8):
            z0, z1 = swap(z[8 * k1 : 8 * k1 + 8], z[64 + 8 * k1 : 64 + 8 * k1 + 8], low)
            x_s[rows_at((kr * 8 + k1) * 64 + br * 8, 8), :] = z0
            x_s[rows_at((kr * 8 + 8 + k1) * 64 + br * 8, 8), :] = z1

    sweep(0, put0, turn)
    loop(64 // G, UB, lambda i: bra_group(1, i * G, [second(i * G + g) for g in range(G)]))

    def put1(b, y):
        bd, br = b // 8, b % 8
        for kd in range(8):
            s_s[pl.ds(kd * 8 + bd + br * 8 * BS, 8, stride=BS), :] = y[8 * kd : 8 * (kd + 1)]

    def leave(i):
        br, kr = i // 4, 2 * (i % 4)
        z = turned(i)
        for e in range(2):
            for r in range(4):
                z0, z1 = swap(z[64 * e + 8 * r : 64 * e + 8 * r + 8], z[64 * e + 32 + 8 * r : 64 * e + 40 + 8 * r], low)
                h, row = r // 2, 16 * e + 8 * (r % 2)
                out[2 * (kr * 8 + br) + h, row : row + 8, :] = z0
                out[2 * (kr * 8 + 8 + br) + h, row : row + 8, :] = z1

    sweep(1, put1, leave)


HBM = pl.BlockSpec(memory_space=pltpu.HBM)
VMEM = pl.BlockSpec(memory_space=pltpu.VMEM)


def absorb(env, p, ops):
    return pl.pallas_call(
        absorb_kernel,
        out_shape=jax.ShapeDtypeStruct((128, 32, 128), F32),
        in_specs=[HBM, HBM, HBM],
        out_specs=VMEM,
        scratch_shapes=[
            pltpu.VMEM((2, 1, 64, 4096), F32),
            pltpu.VMEM((256, 8, 8), F32),
            pltpu.VMEM((8, 256, 8), F32),
            pltpu.SMEM((2, 2, 2), F32),
            pltpu.VMEM((4096, 128), F32),
            pltpu.VMEM((64 * RS, 128), F32),
            pltpu.VMEM((64 * BS, 128), F32),
            pltpu.VMEM((2, 128, 192), BF16),
            pltpu.VMEM((2, 128, 256), BF16),
            pltpu.SemaphoreType.DMA((8,)),
            pltpu.SemaphoreType.DMA,
            pltpu.SemaphoreType.DMA,
        ],
        compiler_params=pltpu.CompilerParams(vmem_limit_bytes=40 << 20),
        cost_estimate=pl.CostEstimate(flops=2 << 30, bytes_accessed=4 << 20, transcendentals=0),
        name="absorb",
    )(env, p, ops)


def absorb_raw(env, peps, ops):
    return absorb(*[pltpu.with_memory_space_constraint(v, pltpu.HBM) for v in (env, peps.reshape(256, 8, 8), ops)])


def gauge_kernel(r, gm, out, sq, w_s):
    hi, lo = halves(gm[...])
    w_s[...] = jnp.concatenate([hi, hi, lo], axis=1)
    lane = lax.broadcasted_iota(jnp.int32, (1, 128), 1)
    row = jnp.zeros((1, 128), F32)
    w = w_s[...]
    for e in range(2):
        tot = jnp.zeros((8, 128), F32)
        for b in range(0, 16, 4):
            x = jnp.concatenate([r[pl.ds(e * 16 + b + g, 128, stride=32), :] for g in range(4)], axis=1)
            y = mm(w, x)
            out[e, :, 128 * b : 128 * (b + 4)] = y
            q = (y * y).reshape(16, 8, 512).sum(0)
            for g in range(4):
                tot = tot + q[:, 128 * g : 128 * (g + 1)]
        row = jnp.where(lane == e, jnp.sum(tot), row)
    sq[...] = jnp.broadcast_to(row[None], (128, 1, 128))


def gauge(r, gm):
    return pl.pallas_call(
        gauge_kernel,
        out_shape=(jax.ShapeDtypeStruct((2, 128, 2048), F32), jax.ShapeDtypeStruct((128, 1, 128), F32)),
        in_specs=[VMEM, VMEM],
        out_specs=(VMEM, VMEM),
        scratch_shapes=[pltpu.VMEM((128, 384), BF16)],
        compiler_params=pltpu.CompilerParams(vmem_limit_bytes=40 << 20),
        cost_estimate=pl.CostEstimate(flops=1 << 29, bytes_accessed=4 << 20, transcendentals=0),
        name="gauge",
    )(r.reshape(4096, 128), gm)


def scale_kernel(entries, x, sums, out, rms, y_s, sems):
    total = jnp.sum(sums[...], axis=0)
    lane = lax.broadcasted_iota(jnp.int32, (1, 128), 1)
    copies = []
    for e in range(2):
        mean = jnp.sum(jnp.where(lane == e, total, 0.0), axis=1, keepdims=True) / entries
        factor = lax.rsqrt(mean + EPS)
        for c in range(8):
            at = pl.ds(16 * c, 16)
            y_s[e, at, :] = x[e, at, :] * factor
            copy = pltpu.make_async_copy(y_s.at[e, at, :], out.at[e, at, :], sems.at[8 * e + c])
            copy.start()
            copies.append(copy)
        rms[e] = jnp.sqrt(mean)[0, 0]
    for copy in copies:
        copy.wait()


def scale(x, sums, entries):
    return pl.pallas_call(
        functools.partial(scale_kernel, entries),
        out_shape=(jax.ShapeDtypeStruct((2, 128, 2048), F32), jax.ShapeDtypeStruct((2,), F32)),
        in_specs=[VMEM, VMEM],
        out_specs=(HBM, pl.BlockSpec(memory_space=pltpu.SMEM)),
        scratch_shapes=[pltpu.VMEM((2, 128, 2048), F32), pltpu.SemaphoreType.DMA((16,))],
        compiler_params=pltpu.CompilerParams(vmem_limit_bytes=40 << 20),
        cost_estimate=pl.CostEstimate(flops=1 << 19, bytes_accessed=4 << 20, transcendentals=0),
        name="scale",
    )(x, sums)


def body(environment, peps, operators, gauge_matrix):
    blocks = absorb_raw(environment, peps, operators)
    merged = lax.all_to_all(blocks, BITS, 0, 0, tiled=True)
    gauged, sums = gauge(merged, gauge_matrix)
    sums = lax.all_to_all(sums, BITS, 0, 0, tiled=True)
    entries = gauged.shape[1] * gauged.shape[2] * lax.axis_size(BITS)
    return scale(gauged, sums, entries)


def solution(mesh):
    torus = Mesh(mesh.devices.reshape(4, 4, 4, 2), BITS)
    in_specs = (P(None, BITS, None, None), P(), P(), P())
    out_specs = (P(None, None, BITS), P())
    return jax.shard_map(body, mesh=torus, in_specs=in_specs, out_specs=out_specs, check_vma=False)
```

```python
import functools

import jax
import jax.numpy as jnp
from jax import lax
from jax.experimental import pallas as pl
from jax.experimental.pallas import tpu as pltpu
from jax.sharding import Mesh
from jax.sharding import PartitionSpec as P

BITS = ("bits_0", "bits_1", "bits_2", "bits_3")
EPS = 1e-06
F32, BF16 = jnp.float32, jnp.bfloat16
RS = 132
BS = 68
G = 4
W0 = 8
UB = 16
UBR = 8
KM = 1


def halves(x):
    hi = x.astype(BF16)
    return hi, (x - hi.astype(F32)).astype(BF16)


def tall(x):
    hi, lo = halves(x)
    return jnp.concatenate([hi, lo, hi], axis=0)


def mm(w, x):
    return jnp.dot(w, tall(x), preferred_element_type=F32)


def loop(count, unroll, step):
    def several(i, carry):
        for u in range(unroll):
            step(i * unroll + u)
        return carry

    if unroll == count:
        several(0, 0)
    else:
        lax.fori_loop(0, count // unroll, several, 0)


def rows_at(at, size):
    return pl.ds(at if isinstance(at, int) else pl.multiple_of(at, 8), size)


def swap(a, b, low):
    return jnp.where(low, a, pltpu.roll(b, 64, 1)), jnp.where(low, pltpu.roll(a, 64, 1), b)


def absorb_kernel(env, p, ops, out, env_s, p_s, q_s, ops_s, x_s, t_s, s_s, bra_w, ket_w, env_sem, p_sem, ops_sem):
    small = [pltpu.make_async_copy(p, p_s, p_sem), pltpu.make_async_copy(ops, ops_s, ops_sem)]
    for copy in small:
        copy.start()

    def chunk(kl):
        rows = pl.ds(8 * kl, 8)
        return pltpu.make_async_copy(env.at[:, :, rows, :], env_s.at[:, :, rows, :], env_sem.at[kl])

    for kl in range(8):
        chunk(kl).start(priority=1)
    low = lax.broadcasted_iota(jnp.int32, (8, 128), 1) < 64
    for copy in small:
        copy.wait()
    for g in range(32):
        q_s[:, 8 * g : 8 * g + 8, :] = jnp.swapaxes(p_s[8 * g : 8 * g + 8], 0, 1)
    row = lax.broadcasted_iota(jnp.int32, (64, 64), 0)
    col = lax.broadcasted_iota(jnp.int32, (64, 64), 1)
    exchange = jnp.where(row == (col % 8) * 8 + col // 8, 1.0, 0.0).astype(BF16)
    for j in range(2):
        wj = jnp.concatenate([q_s[d, 128 * j : 128 * (j + 1), :].T for d in range(8)], axis=0)
        hi, lo = halves(wj)
        ket_w[j, :64] = jnp.concatenate([hi, hi], axis=1)
        ket_w[j, 64:] = jnp.concatenate([lo, jnp.zeros_like(lo)], axis=1)
        for a in range(2):
            parts = halves(ops_s[j, a, 0] * wj[:, :64] + ops_s[j, a, 1] * wj[:, 64:])
            if j == 0:
                parts = [jnp.dot(part, exchange, preferred_element_type=F32).astype(BF16) for part in parts]
            hi, lo = parts
            bra_w[j, 64 * a : 64 * (a + 1), :] = jnp.concatenate([hi, hi, lo], axis=1)

    def first(kl, k0):
        rows = rows_at(8 * kl, 8)
        pieces = []
        for c in range(4):
            lanes = pl.ds(k0 * 512 + 128 * c, 128)
            pieces += swap(env_s[0, 0, rows, lanes], env_s[1, 0, rows, lanes], low)
        return jnp.concatenate(pieces, axis=0)

    def second(at):
        return x_s[rows_at(at * 64, 64), :]

    def bra_group(j, at, xs):
        y = mm(bra_w[j], jnp.concatenate(xs, axis=1))
        for g in range(G):
            for a in range(2):
                t_s[pl.ds(a * 64 + at + g, 64, stride=RS), :] = y[64 * a : 64 * (a + 1), 128 * g : 128 * (g + 1)]

    for start in range(0, 8, W0):
        for kl in range(start, start + W0):
            chunk(kl).wait()
        for kl in range(start, start + W0):
            for k0 in range(0, 8, G):
                bra_group(0, kl * 8 + k0, [first(kl, k0 + g) for g in range(G)])

    def ket(j, br, put):
        for start in range(0, 8, G):
            x = jnp.concatenate([t_s[pl.ds(((start + g) * 8 + br) * RS, 128), :] for g in range(G)], axis=1)
            x = jnp.concatenate(halves(x), axis=0)
            if KM:
                y = jnp.dot(ket_w[j], x, preferred_element_type=F32)
                y = y[:64] + y[64:]
            else:
                y = jnp.dot(ket_w[j, :64], x, preferred_element_type=F32) + jnp.dot(ket_w[j, 64:], x, preferred_element_type=F32)
            for g in range(G):
                put((start + g) * 8 + br, y[:, 128 * g : 128 * (g + 1)])

    def put0(b, y):
        bd, br = b // 8, b % 8
        for kd in range(8):
            s_s[pl.ds(br * 8 * BS + (bd % 2) * 32 + kd * 4 + bd // 2, 8, stride=BS), :] = y[8 * kd : 8 * (kd + 1)]

    def turned(i):
        return jnp.concatenate([s_s[pl.ds(2 * i * BS, 64), :], s_s[pl.ds((2 * i + 1) * BS, 64), :]], axis=0).T

    def sweep(j, put, finish):
        def step(br):
            ket(j, br, put)
            for i in range(4):
                finish(br * 4 + i)

        loop(8, UBR, step)

    def turn(i):
        br, kr = i // 4, 2 * (i % 4)
        z = turned(i)
        for k1 in range(8):
            z0, z1 = swap(z[8 * k1 : 8 * k1 + 8], z[64 + 8 * k1 : 64 + 8 * k1 + 8], low)
            x_s[rows_at((kr * 8 + k1) * 64 + br * 8, 8), :] = z0
            x_s[rows_at((kr * 8 + 8 + k1) * 64 + br * 8, 8), :] = z1

    sweep(0, put0, turn)
    loop(64 // G, UB, lambda i: bra_group(1, i * G, [second(i * G + g) for g in range(G)]))

    def put1(b, y):
        bd, br = b // 8, b % 8
        for kd in range(8):
            s_s[pl.ds(kd * 8 + bd + br * 8 * BS, 8, stride=BS), :] = y[8 * kd : 8 * (kd + 1)]

    def leave(i):
        br, kr = i // 4, 2 * (i % 4)
        z = turned(i)
        for e in range(2):
            for r in range(4):
                z0, z1 = swap(z[64 * e + 8 * r : 64 * e + 8 * r + 8], z[64 * e + 32 + 8 * r : 64 * e + 40 + 8 * r], low)
                h, row = r // 2, 16 * e + 8 * (r % 2)
                out[2 * (kr * 8 + br) + h, row : row + 8, :] = z0
                out[2 * (kr * 8 + 8 + br) + h, row : row + 8, :] = z1

    sweep(1, put1, leave)


HBM = pl.BlockSpec(memory_space=pltpu.HBM)
VMEM = pl.BlockSpec(memory_space=pltpu.VMEM)


def absorb(env, p, ops):
    return pl.pallas_call(
        absorb_kernel,
        out_shape=jax.ShapeDtypeStruct((128, 32, 128), F32),
        in_specs=[HBM, HBM, HBM],
        out_specs=VMEM,
        scratch_shapes=[
            pltpu.VMEM((2, 1, 64, 4096), F32),
            pltpu.VMEM((256, 8, 8), F32),
            pltpu.VMEM((8, 256, 8), F32),
            pltpu.SMEM((2, 2, 2), F32),
            pltpu.VMEM((4096, 128), F32),
            pltpu.VMEM((64 * RS, 128), F32),
            pltpu.VMEM((64 * BS, 128), F32),
            pltpu.VMEM((2, 128, 192), BF16),
            pltpu.VMEM((2, 128, 256), BF16),
            pltpu.SemaphoreType.DMA((8,)),
            pltpu.SemaphoreType.DMA,
            pltpu.SemaphoreType.DMA,
        ],
        compiler_params=pltpu.CompilerParams(vmem_limit_bytes=40 << 20),
        cost_estimate=pl.CostEstimate(flops=2 << 30, bytes_accessed=4 << 20, transcendentals=0),
        name="absorb",
    )(env, p, ops)


def absorb_raw(env, peps, ops):
    return absorb(*[pltpu.with_memory_space_constraint(v, pltpu.HBM) for v in (env, peps.reshape(256, 8, 8), ops)])


def gauge_kernel(r, gm, out, sq, w_s, x_s):
    hi, lo = halves(gm[...])
    w_s[:128] = jnp.concatenate([hi, hi], axis=1)
    w_s[128:] = jnp.concatenate([lo, jnp.zeros_like(lo)], axis=1)
    for t in range(4):
        for m in range(16):
            part = jnp.swapaxes(r[8 * m : 8 * m + 8, 8 * t : 8 * t + 8, :], 0, 1)
            for s in range(8):
                x_s[8 * t + s, 8 * m : 8 * m + 8, :] = part[s]
    low = lax.broadcasted_iota(jnp.int32, (1, 128), 1) < 64
    sums = []
    for e in range(2):
        tot = jnp.zeros((8, 128), F32)
        for b in range(0, 16, 4):
            x = jnp.concatenate([x_s[e * 16 + b + g] for g in range(4)], axis=1)
            y = jnp.dot(w_s[...], jnp.concatenate(halves(x), axis=0), preferred_element_type=F32)
            y = y[:128] + y[128:]
            out[e, :, 128 * b : 128 * (b + 4)] = y
            q = (y * y).reshape(16, 8, 512).sum(0)
            for g in range(4):
                tot = tot + q[:, 128 * g : 128 * (g + 1)]
        sums.append(jnp.sum(tot))
    sq[...] = jnp.broadcast_to(jnp.where(low, sums[0], sums[1]), (128, 128))


def gauge(r, gm):
    return pl.pallas_call(
        gauge_kernel,
        out_shape=(jax.ShapeDtypeStruct((2, 128, 2048), F32), jax.ShapeDtypeStruct((128, 128), F32)),
        in_specs=[VMEM, VMEM],
        out_specs=(VMEM, VMEM),
        scratch_shapes=[pltpu.VMEM((256, 256), BF16), pltpu.VMEM((32, 128, 128), F32)],
        compiler_params=pltpu.CompilerParams(vmem_limit_bytes=40 << 20),
        cost_estimate=pl.CostEstimate(flops=1 << 29, bytes_accessed=4 << 20, transcendentals=0),
        name="gauge",
    )(r, gm)


def scale_kernel(entries, x, sums, out, rms, y_s, sems):
    total = jnp.sum(sums[...], axis=0, keepdims=True)
    low = lax.broadcasted_iota(jnp.int32, (1, 128), 1) < 64
    other = pltpu.roll(total, 64, 1)
    copies = []
    means = [jnp.where(low, total, other) / entries, jnp.where(low, other, total) / entries]
    for e in range(2):
        factor = jnp.concatenate([lax.rsqrt(means[e] + EPS)] * 16, axis=1)
        for c in range(4):
            at = pl.ds(128 // 4 * c, 128 // 4)
            y_s[e, at, :] = x[e, at, :] * factor
            copy = pltpu.make_async_copy(y_s.at[e, at, :], out.at[e, at, :], sems.at[4 * e + c])
            copy.start()
            copies.append(copy)
    for e in range(2):
        rms[e] = jnp.sqrt(means[e])[0, 0]
    for copy in copies:
        copy.wait()


def scale(x, sums, entries):
    return pl.pallas_call(
        functools.partial(scale_kernel, entries),
        out_shape=(jax.ShapeDtypeStruct((2, 128, 2048), F32), jax.ShapeDtypeStruct((2,), F32)),
        in_specs=[VMEM, VMEM],
        out_specs=(HBM, pl.BlockSpec(memory_space=pltpu.SMEM)),
        scratch_shapes=[pltpu.VMEM((2, 128, 2048), F32), pltpu.SemaphoreType.DMA((2 * 4,))],
        compiler_params=pltpu.CompilerParams(vmem_limit_bytes=40 << 20),
        cost_estimate=pl.CostEstimate(flops=1 << 19, bytes_accessed=4 << 20, transcendentals=0),
        name="scale",
    )(x, sums)


def body(environment, peps, operators, gauge_matrix):
    blocks = absorb_raw(environment, peps, operators)
    merged = lax.all_to_all(blocks, BITS, 0, 0, tiled=True)
    gauged, sums = gauge(merged, gauge_matrix)
    sums = lax.all_to_all(sums, BITS, 0, 0, tiled=True)
    entries = gauged.shape[1] * gauged.shape[2] * lax.axis_size(BITS)
    return scale(gauged, sums, entries)


def solution(mesh):
    torus = Mesh(mesh.devices.reshape(4, 4, 4, 2), BITS)
    in_specs = (P(None, BITS, None, None), P(), P(), P())
    out_specs = (P(None, None, BITS), P())
    return jax.shard_map(body, mesh=torus, in_specs=in_specs, out_specs=out_specs, check_vma=False)
```

```python
import functools

import jax
import jax.numpy as jnp
from jax import lax
from jax.experimental import pallas as pl
from jax.experimental.pallas import tpu as pltpu
from jax.sharding import Mesh
from jax.sharding import PartitionSpec as P

BITS = ("bits_0", "bits_1", "bits_2", "bits_3")
EPS = 1e-06
F32, BF16 = jnp.float32, jnp.bfloat16
RS = 132
BS = 68
G = 4
W0 = 8
UB = 16
UBR = 8
KM = 1
LATE = 1


def halves(x):
    hi = x.astype(BF16)
    return hi, (x - hi.astype(F32)).astype(BF16)


def tall(x):
    hi, lo = halves(x)
    return jnp.concatenate([hi, lo, hi], axis=0)


def mm(w, x):
    return jnp.dot(w, tall(x), preferred_element_type=F32)


def loop(count, unroll, step):
    def several(i, carry):
        for u in range(unroll):
            step(i * unroll + u)
        return carry

    if unroll == count:
        several(0, 0)
    else:
        lax.fori_loop(0, count // unroll, several, 0)


def rows_at(at, size):
    return pl.ds(at if isinstance(at, int) else pl.multiple_of(at, 8), size)


def swap(a, b, low):
    return jnp.where(low, a, pltpu.roll(b, 64, 1)), jnp.where(low, pltpu.roll(a, 64, 1), b)


def absorb_kernel(env, p, ops, out, env_s, p_s, q_s, ops_s, x_s, t_s, s_s, bra_w, ket_w, env_sem, p_sem, ops_sem):
    small = [pltpu.make_async_copy(p, p_s, p_sem), pltpu.make_async_copy(ops, ops_s, ops_sem)]
    for copy in small:
        copy.start()

    def chunk(kl):
        rows = pl.ds(8 * kl, 8)
        return pltpu.make_async_copy(env.at[:, :, rows, :], env_s.at[:, :, rows, :], env_sem.at[kl])

    for kl in range(8):
        chunk(kl).start(priority=1)
    low = lax.broadcasted_iota(jnp.int32, (8, 128), 1) < 64
    for copy in small:
        copy.wait()
    def weights(j):
        for g in range(16):
            part = pl.ds(64 * (g // 8) + g % 8, 8, stride=8) if j == 0 else pl.ds(128 + 8 * g, 8)
            q_s[:, 128 * j + 8 * g : 128 * j + 8 * g + 8, :] = jnp.swapaxes(p_s[part], 0, 1)
        w = jnp.concatenate([q_s[d, 128 * j : 128 * (j + 1), :].T for d in range(8)], axis=0)
        for a in range(2):
            hi, lo = halves(ops_s[j, a, 0] * w[:, :64] + ops_s[j, a, 1] * w[:, 64:])
            bra_w[j, 64 * a : 64 * (a + 1), :] = jnp.concatenate([hi, hi, lo], axis=1)
        hi, lo = halves(w)
        ket_w[j, :64] = jnp.concatenate([hi, hi], axis=1)
        ket_w[j, 64:] = jnp.concatenate([lo, jnp.zeros_like(lo)], axis=1)

    weights(0)
    if not LATE:
        weights(1)

    def first(kl, k0):
        rows = rows_at(8 * kl, 8)
        pieces = []
        for c in range(4):
            lanes = pl.ds(k0 * 512 + 128 * c, 128)
            pieces += swap(env_s[0, 0, rows, lanes], env_s[1, 0, rows, lanes], low)
        return jnp.concatenate(pieces, axis=0)

    def second(at):
        return x_s[rows_at(at * 64, 64), :]

    def bra_group(j, places, xs):
        y = mm(bra_w[j], jnp.concatenate(xs, axis=1))
        for g in range(G):
            for a in range(2):
                t_s[pl.ds(a * 64 + places[g], 64, stride=RS), :] = y[64 * a : 64 * (a + 1), 128 * g : 128 * (g + 1)]

    for start in range(0, 8, W0):
        for kl in range(start, start + W0):
            chunk(kl).wait()
        for kl in range(start, start + W0):
            for k0 in range(0, 8, G):
                bra_group(0, [(k0 + g) * 8 + kl for g in range(G)], [first(kl, k0 + g) for g in range(G)])

    def ket(j, br, put):
        for start in range(0, 8, G):
            x = jnp.concatenate([t_s[pl.ds(((start + g) * 8 + br) * RS, 128), :] for g in range(G)], axis=1)
            x = jnp.concatenate(halves(x), axis=0)
            if KM:
                y = jnp.dot(ket_w[j], x, preferred_element_type=F32)
                y = y[:64] + y[64:]
            else:
                y = jnp.dot(ket_w[j, :64], x, preferred_element_type=F32) + jnp.dot(ket_w[j, 64:], x, preferred_element_type=F32)
            for g in range(G):
                put((start + g) * 8 + br, y[:, 128 * g : 128 * (g + 1)])

    def put0(b, y):
        bd, br = b // 8, b % 8
        for kd in range(8):
            s_s[pl.ds(br * 8 * BS + (bd % 2) * 32 + kd * 4 + bd // 2, 8, stride=BS), :] = y[8 * kd : 8 * (kd + 1)]

    def turned(i):
        return jnp.concatenate([s_s[pl.ds(2 * i * BS, 64), :], s_s[pl.ds((2 * i + 1) * BS, 64), :]], axis=0).T

    def sweep(j, put, finish):
        def step(br):
            ket(j, br, put)
            for i in range(4):
                finish(br * 4 + i)

        loop(8, UBR, step)

    def turn(i):
        br, kr = i // 4, 2 * (i % 4)
        z = turned(i)
        for k1 in range(8):
            z0, z1 = swap(z[8 * k1 : 8 * k1 + 8], z[64 + 8 * k1 : 64 + 8 * k1 + 8], low)
            x_s[rows_at((kr * 8 + k1) * 64 + br * 8, 8), :] = z0
            x_s[rows_at((kr * 8 + 8 + k1) * 64 + br * 8, 8), :] = z1

    if LATE:
        weights(1)
    sweep(0, put0, turn)
    loop(64 // G, UB, lambda i: bra_group(1, [i * G + g for g in range(G)], [second(i * G + g) for g in range(G)]))

    def put1(b, y):
        bd, br = b // 8, b % 8
        for kd in range(8):
            s_s[pl.ds(kd * 8 + bd + br * 8 * BS, 8, stride=BS), :] = y[8 * kd : 8 * (kd + 1)]

    def leave(i):
        br, kr = i // 4, 2 * (i % 4)
        z = turned(i)
        for e in range(2):
            for r in range(4):
                z0, z1 = swap(z[64 * e + 8 * r : 64 * e + 8 * r + 8], z[64 * e + 32 + 8 * r : 64 * e + 40 + 8 * r], low)
                h, row = r // 2, 16 * e + 8 * (r % 2)
                out[2 * (kr * 8 + br) + h, row : row + 8, :] = z0
                out[2 * (kr * 8 + 8 + br) + h, row : row + 8, :] = z1

    sweep(1, put1, leave)


HBM = pl.BlockSpec(memory_space=pltpu.HBM)
VMEM = pl.BlockSpec(memory_space=pltpu.VMEM)


def absorb(env, p, ops):
    return pl.pallas_call(
        absorb_kernel,
        out_shape=jax.ShapeDtypeStruct((128, 32, 128), F32),
        in_specs=[HBM, HBM, HBM],
        out_specs=VMEM,
        scratch_shapes=[
            pltpu.VMEM((2, 1, 64, 4096), F32),
            pltpu.VMEM((256, 8, 8), F32),
            pltpu.VMEM((8, 256, 8), F32),
            pltpu.SMEM((2, 2, 2), F32),
            pltpu.VMEM((4096, 128), F32),
            pltpu.VMEM((64 * RS, 128), F32),
            pltpu.VMEM((64 * BS, 128), F32),
            pltpu.VMEM((2, 128, 192), BF16),
            pltpu.VMEM((2, 128, 256), BF16),
            pltpu.SemaphoreType.DMA((8,)),
            pltpu.SemaphoreType.DMA,
            pltpu.SemaphoreType.DMA,
        ],
        compiler_params=pltpu.CompilerParams(vmem_limit_bytes=40 << 20),
        cost_estimate=pl.CostEstimate(flops=2 << 30, bytes_accessed=4 << 20, transcendentals=0),
        name="absorb",
    )(env, p, ops)


def absorb_raw(env, peps, ops):
    return absorb(*[pltpu.with_memory_space_constraint(v, pltpu.HBM) for v in (env, peps.reshape(256, 8, 8), ops)])


def gauge_kernel(r, gm, out, sq, w_s, x_s):
    hi, lo = halves(gm[...])
    w_s[:128] = jnp.concatenate([hi, hi], axis=1)
    w_s[128:] = jnp.concatenate([lo, jnp.zeros_like(lo)], axis=1)
    for t in range(4):
        for m in range(16):
            part = jnp.swapaxes(r[8 * m : 8 * m + 8, 8 * t : 8 * t + 8, :], 0, 1)
            for s in range(8):
                x_s[8 * t + s, 8 * m : 8 * m + 8, :] = part[s]
    low = lax.broadcasted_iota(jnp.int32, (1, 128), 1) < 64
    sums = []
    for e in range(2):
        tot = jnp.zeros((8, 128), F32)
        for b in range(0, 16, 4):
            x = jnp.concatenate([x_s[e * 16 + b + g] for g in range(4)], axis=1)
            y = jnp.dot(w_s[...], jnp.concatenate(halves(x), axis=0), preferred_element_type=F32)
            y = y[:128] + y[128:]
            out[e, :, 128 * b : 128 * (b + 4)] = y
            q = (y * y).reshape(16, 8, 512).sum(0)
            for g in range(4):
                tot = tot + q[:, 128 * g : 128 * (g + 1)]
        sums.append(jnp.sum(tot))
    sq[...] = jnp.broadcast_to(jnp.where(low, sums[0], sums[1]), (128, 128))


def gauge(r, gm):
    return pl.pallas_call(
        gauge_kernel,
        out_shape=(jax.ShapeDtypeStruct((2, 128, 2048), F32), jax.ShapeDtypeStruct((128, 128), F32)),
        in_specs=[VMEM, VMEM],
        out_specs=(VMEM, VMEM),
        scratch_shapes=[pltpu.VMEM((256, 256), BF16), pltpu.VMEM((32, 128, 128), F32)],
        compiler_params=pltpu.CompilerParams(vmem_limit_bytes=40 << 20),
        cost_estimate=pl.CostEstimate(flops=1 << 29, bytes_accessed=4 << 20, transcendentals=0),
        name="gauge",
    )(r, gm)


def scale_kernel(entries, x, sums, out, rms, y_s, rms_s, sems, rms_sem):
    total = jnp.sum(sums[...], axis=0, keepdims=True)
    low = lax.broadcasted_iota(jnp.int32, (1, 128), 1) < 64
    other = pltpu.roll(total, 64, 1)
    copies = []
    means = [jnp.where(low, total, other) / entries, jnp.where(low, other, total) / entries]
    for e in range(2):
        factor = jnp.concatenate([lax.rsqrt(means[e] + EPS)] * 16, axis=1)
        for c in range(4):
            at = pl.ds(128 // 4 * c, 128 // 4)
            y_s[e, at, :] = x[e, at, :] * factor
            copy = pltpu.make_async_copy(y_s.at[e, at, :], out.at[e, at, :], sems.at[4 * e + c])
            copy.start()
            copies.append(copy)
    for e in range(2):
        rms_s[e] = jnp.sqrt(means[e])[0, 0]
    copy = pltpu.make_async_copy(rms_s, rms, rms_sem)
    copy.start()
    copies.append(copy)
    for copy in copies:
        copy.wait()


def scale(x, sums, entries):
    return pl.pallas_call(
        functools.partial(scale_kernel, entries),
        out_shape=(jax.ShapeDtypeStruct((2, 128, 2048), F32), jax.ShapeDtypeStruct((2,), F32)),
        in_specs=[VMEM, VMEM],
        out_specs=(HBM, HBM),
        scratch_shapes=[
            pltpu.VMEM((2, 128, 2048), F32),
            pltpu.SMEM((2,), F32),
            pltpu.SemaphoreType.DMA((2 * 4,)),
            pltpu.SemaphoreType.DMA,
        ],
        compiler_params=pltpu.CompilerParams(vmem_limit_bytes=40 << 20),
        cost_estimate=pl.CostEstimate(flops=1 << 19, bytes_accessed=4 << 20, transcendentals=0),
        name="scale",
    )(x, sums)


def body(environment, peps, operators, gauge_matrix):
    blocks = absorb_raw(environment, peps, operators)
    merged = lax.all_to_all(blocks, BITS, 0, 0, tiled=True)
    gauged, sums = gauge(merged, gauge_matrix)
    sums = lax.all_to_all(sums, BITS, 0, 0, tiled=True)
    entries = gauged.shape[1] * gauged.shape[2] * lax.axis_size(BITS)
    return scale(gauged, sums, entries)


def solution(mesh):
    torus = Mesh(mesh.devices.reshape(4, 4, 4, 2), BITS)
    in_specs = (P(None, BITS, None, None), P(), P(), P())
    out_specs = (P(None, None, BITS), P())
    return jax.shard_map(body, mesh=torus, in_specs=in_specs, out_specs=out_specs, check_vma=False)
```

```python
import functools

import jax
import jax.numpy as jnp
from jax import lax
from jax.experimental import pallas as pl
from jax.experimental.pallas import tpu as pltpu
from jax.sharding import Mesh
from jax.sharding import PartitionSpec as P

BITS = ("bits_0", "bits_1", "bits_2", "bits_3")
EPS = 1e-06
F32, BF16 = jnp.float32, jnp.bfloat16
RS = 132
BS = 68
G = 4
W0 = 8
UB = 16
UBR = 8
KM = 1
LATE = 1


def halves(x):
    hi = x.astype(BF16)
    return hi, (x - hi.astype(F32)).astype(BF16)


def tall(x):
    hi, lo = halves(x)
    return jnp.concatenate([hi, lo, hi], axis=0)


def mm(w, x):
    return jnp.dot(w, tall(x), preferred_element_type=F32)


def loop(count, unroll, step):
    def several(i, carry):
        for u in range(unroll):
            step(i * unroll + u)
        return carry

    if unroll == count:
        several(0, 0)
    else:
        lax.fori_loop(0, count // unroll, several, 0)


def rows_at(at, size):
    return pl.ds(at if isinstance(at, int) else pl.multiple_of(at, 8), size)


def swap(a, b, low):
    return jnp.where(low, a, pltpu.roll(b, 64, 1)), jnp.where(low, pltpu.roll(a, 64, 1), b)


def absorb_kernel(env, p, ops, out, env_s, p_s, q_s, ops_s, x_s, t_s, s_s, bra_w, ket_w, env_sem, p_sem, ops_sem):
    small = [pltpu.make_async_copy(p, p_s, p_sem), pltpu.make_async_copy(ops, ops_s, ops_sem)]
    for copy in small:
        copy.start()

    def chunk(kl):
        rows = pl.ds(8 * kl, 8)
        return pltpu.make_async_copy(env.at[:, :, rows, :], env_s.at[:, :, rows, :], env_sem.at[kl])

    for kl in range(8):
        chunk(kl).start(priority=1)
    low = lax.broadcasted_iota(jnp.int32, (8, 128), 1) < 64
    for copy in small:
        copy.wait()
    def weights(j):
        for g in range(16):
            part = pl.ds(64 * (g // 8) + g % 8, 8, stride=8) if j == 0 else pl.ds(128 + 8 * g, 8)
            q_s[:, 128 * j + 8 * g : 128 * j + 8 * g + 8, :] = jnp.swapaxes(p_s[part], 0, 1)
        w = jnp.concatenate([q_s[d, 128 * j : 128 * (j + 1), :].T for d in range(8)], axis=0)
        for a in range(2):
            hi, lo = halves(ops_s[j, a, 0] * w[:, :64] + ops_s[j, a, 1] * w[:, 64:])
            bra_w[j, 64 * a : 64 * (a + 1), :] = jnp.concatenate([hi, hi, lo], axis=1)
        hi, lo = halves(w)
        ket_w[j, :64] = jnp.concatenate([hi, hi], axis=1)
        ket_w[j, 64:] = jnp.concatenate([lo, jnp.zeros_like(lo)], axis=1)

    weights(0)
    if not LATE:
        weights(1)

    def first(kl, k0):
        rows = rows_at(8 * kl, 8)
        pieces = []
        for c in range(4):
            lanes = pl.ds(k0 * 512 + 128 * c, 128)
            pieces += swap(env_s[0, 0, rows, lanes], env_s[1, 0, rows, lanes], low)
        return jnp.concatenate(pieces, axis=0)

    def second(at):
        return x_s[rows_at(at * 64, 64), :]

    def bra_group(j, places, xs):
        y = mm(bra_w[j], jnp.concatenate(xs, axis=1))
        for g in range(G):
            for a in range(2):
                t_s[pl.ds(a * 64 + places[g], 64, stride=RS), :] = y[64 * a : 64 * (a + 1), 128 * g : 128 * (g + 1)]

    for start in range(0, 8, W0):
        for kl in range(start, start + W0):
            chunk(kl).wait()
        for kl in range(start, start + W0):
            for k0 in range(0, 8, G):
                bra_group(0, [(k0 + g) * 8 + kl for g in range(G)], [first(kl, k0 + g) for g in range(G)])

    def ket(j, br, put):
        for start in range(0, 8, G):
            x = jnp.concatenate([t_s[pl.ds(((start + g) * 8 + br) * RS, 128), :] for g in range(G)], axis=1)
            x = jnp.concatenate(halves(x), axis=0)
            if KM:
                y = jnp.dot(ket_w[j], x, preferred_element_type=F32)
                y = y[:64] + y[64:]
            else:
                y = jnp.dot(ket_w[j, :64], x, preferred_element_type=F32) + jnp.dot(ket_w[j, 64:], x, preferred_element_type=F32)
            for g in range(G):
                put((start + g) * 8 + br, y[:, 128 * g : 128 * (g + 1)])

    def put0(b, y):
        bd, br = b // 8, b % 8
        for kd in range(8):
            s_s[pl.ds(br * 8 * BS + (bd % 2) * 32 + kd * 4 + bd // 2, 8, stride=BS), :] = y[8 * kd : 8 * (kd + 1)]

    def turned(i):
        return jnp.concatenate([s_s[pl.ds(2 * i * BS, 64), :], s_s[pl.ds((2 * i + 1) * BS, 64), :]], axis=0).T

    def sweep(j, put, finish):
        def step(br):
            ket(j, br, put)
            for i in range(4):
                finish(br * 4 + i)

        loop(8, UBR, step)

    def turn(i):
        br, kr = i // 4, 2 * (i % 4)
        z = turned(i)
        for k1 in range(8):
            z0, z1 = swap(z[8 * k1 : 8 * k1 + 8], z[64 + 8 * k1 : 64 + 8 * k1 + 8], low)
            x_s[rows_at((kr * 8 + k1) * 64 + br * 8, 8), :] = z0
            x_s[rows_at((kr * 8 + 8 + k1) * 64 + br * 8, 8), :] = z1

    if LATE:
        weights(1)
    sweep(0, put0, turn)
    loop(64 // G, UB, lambda i: bra_group(1, [i * G + g for g in range(G)], [second(i * G + g) for g in range(G)]))

    def put1(b, y):
        bd, br = b // 8, b % 8
        for kd in range(8):
            s_s[pl.ds(kd * 8 + bd + br * 8 * BS, 8, stride=BS), :] = y[8 * kd : 8 * (kd + 1)]

    def leave(i):
        br, kr = i // 4, 2 * (i % 4)
        z = turned(i)
        for e in range(2):
            for r in range(4):
                z0, z1 = swap(z[64 * e + 8 * r : 64 * e + 8 * r + 8], z[64 * e + 32 + 8 * r : 64 * e + 40 + 8 * r], low)
                h, row = r // 2, 16 * e + 8 * (r % 2)
                out[2 * (kr * 8 + br) + h, row : row + 8, :] = z0
                out[2 * (kr * 8 + 8 + br) + h, row : row + 8, :] = z1

    sweep(1, put1, leave)


HBM = pl.BlockSpec(memory_space=pltpu.HBM)
VMEM = pl.BlockSpec(memory_space=pltpu.VMEM)


def absorb(env, p, ops):
    return pl.pallas_call(
        absorb_kernel,
        out_shape=jax.ShapeDtypeStruct((128, 32, 128), F32),
        in_specs=[HBM, HBM, HBM],
        out_specs=VMEM,
        scratch_shapes=[
            pltpu.VMEM((2, 1, 64, 4096), F32),
            pltpu.VMEM((256, 8, 8), F32),
            pltpu.VMEM((8, 256, 8), F32),
            pltpu.SMEM((2, 2, 2), F32),
            pltpu.VMEM((4096, 128), F32),
            pltpu.VMEM((64 * RS, 128), F32),
            pltpu.VMEM((64 * BS, 128), F32),
            pltpu.VMEM((2, 128, 192), BF16),
            pltpu.VMEM((2, 128, 256), BF16),
            pltpu.SemaphoreType.DMA((8,)),
            pltpu.SemaphoreType.DMA,
            pltpu.SemaphoreType.DMA,
        ],
        compiler_params=pltpu.CompilerParams(vmem_limit_bytes=40 << 20),
        cost_estimate=pl.CostEstimate(flops=2 << 30, bytes_accessed=4 << 20, transcendentals=0),
        name="absorb",
    )(env, p, ops)


def absorb_raw(env, peps, ops):
    return absorb(*[pltpu.with_memory_space_constraint(v, pltpu.HBM) for v in (env, peps.reshape(256, 8, 8), ops)])


def gauge_kernel(r, gm, out, sq, w_s, x_s):
    hi, lo = halves(gm[...])
    w_s[:128] = jnp.concatenate([hi, hi], axis=1)
    w_s[128:] = jnp.concatenate([lo, jnp.zeros_like(lo)], axis=1)
    low = lax.broadcasted_iota(jnp.int32, (1, 128), 1) < 64
    sums = []
    for e in range(2):
        tot = jnp.zeros((8, 128), F32)
        for t in (2 * e, 2 * e + 1):
            for m in range(16):
                part = jnp.swapaxes(r[8 * m : 8 * m + 8, 8 * t : 8 * t + 8, :], 0, 1)
                for s in range(8):
                    x_s[8 * t + s, 8 * m : 8 * m + 8, :] = part[s]
            for b in range(8 * t, 8 * t + 8, 4):
                x = jnp.concatenate([x_s[b + g] for g in range(4)], axis=1)
                y = jnp.dot(w_s[...], jnp.concatenate(halves(x), axis=0), preferred_element_type=F32)
                y = y[:128] + y[128:]
                out[e, :, 128 * (b - 16 * e) : 128 * (b - 16 * e + 4)] = y
                q = (y * y).reshape(16, 8, 128 * 4).sum(0)
                for g in range(4):
                    tot = tot + q[:, 128 * g : 128 * (g + 1)]
        part = jnp.sum(tot, axis=0, keepdims=True)
        sums.append(part + pltpu.roll(part, 64, 1))
    sq[...] = jnp.broadcast_to(jnp.where(low, sums[0], sums[1]), (128, 128))


def gauge(r, gm):
    return pl.pallas_call(
        gauge_kernel,
        out_shape=(jax.ShapeDtypeStruct((2, 128, 2048), F32), jax.ShapeDtypeStruct((128, 128), F32)),
        in_specs=[VMEM, VMEM],
        out_specs=(VMEM, VMEM),
        scratch_shapes=[pltpu.VMEM((256, 256), BF16), pltpu.VMEM((32, 128, 128), F32)],
        compiler_params=pltpu.CompilerParams(vmem_limit_bytes=40 << 20),
        cost_estimate=pl.CostEstimate(flops=1 << 29, bytes_accessed=4 << 20, transcendentals=0),
        name="gauge",
    )(r, gm)


def scale_kernel(entries, x, sums, out, rms, y_s, rms_s, sems, rms_sem):
    total = jnp.sum(sums[...], axis=0, keepdims=True)
    low = lax.broadcasted_iota(jnp.int32, (1, 128), 1) < 64
    copies = []
    means = [jnp.sum(jnp.where(half, total, 0.0), axis=1, keepdims=True) / entries for half in (low, ~low)]
    for e in range(2):
        factor = lax.rsqrt(means[e] + EPS)
        for c in range(4):
            at = pl.ds(128 // 4 * c, 128 // 4)
            y_s[e, at, :] = x[e, at, :] * factor
            copy = pltpu.make_async_copy(y_s.at[e, at, :], out.at[e, at, :], sems.at[4 * e + c])
            copy.start()
            copies.append(copy)
    for e in range(2):
        rms_s[e] = jnp.sqrt(means[e])[0, 0]
    copy = pltpu.make_async_copy(rms_s, rms, rms_sem)
    copy.start()
    copies.append(copy)
    for copy in copies:
        copy.wait()


def scale(x, sums, entries):
    return pl.pallas_call(
        functools.partial(scale_kernel, entries),
        out_shape=(jax.ShapeDtypeStruct((2, 128, 2048), F32), jax.ShapeDtypeStruct((2,), F32)),
        in_specs=[VMEM, VMEM],
        out_specs=(HBM, HBM),
        scratch_shapes=[
            pltpu.VMEM((2, 128, 2048), F32),
            pltpu.SMEM((2,), F32),
            pltpu.SemaphoreType.DMA((2 * 4,)),
            pltpu.SemaphoreType.DMA,
        ],
        compiler_params=pltpu.CompilerParams(vmem_limit_bytes=40 << 20),
        cost_estimate=pl.CostEstimate(flops=1 << 19, bytes_accessed=4 << 20, transcendentals=0),
        name="scale",
    )(x, sums)


def body(environment, peps, operators, gauge_matrix):
    blocks = absorb_raw(environment, peps, operators)
    merged = lax.all_to_all(blocks, BITS, 0, 0, tiled=True)
    gauged, sums = gauge(merged, gauge_matrix)
    sums = lax.all_to_all(sums, BITS, 0, 0, tiled=True)
    entries = gauged.shape[1] * gauged.shape[2] * lax.axis_size(BITS)
    return scale(gauged, sums, entries)


def solution(mesh):
    torus = Mesh(mesh.devices.reshape(4, 4, 4, 2), BITS)
    in_specs = (P(None, BITS, None, None), P(), P(), P())
    out_specs = (P(None, None, BITS), P())
    return jax.shard_map(body, mesh=torus, in_specs=in_specs, out_specs=out_specs, check_vma=False)
```

```python
import functools

import jax
import jax.numpy as jnp
from jax import lax
from jax.experimental import pallas as pl
from jax.experimental.pallas import tpu as pltpu
from jax.sharding import Mesh
from jax.sharding import PartitionSpec as P

BITS = ("bits_0", "bits_1", "bits_2", "bits_3")
EPS = 1e-06
F32, BF16 = jnp.float32, jnp.bfloat16
RS = 132
BS = 68
G = 4
W0 = 8
UB = 16
UBR = 8
KM = 1
LATE = 1


def halves(x):
    hi = x.astype(BF16)
    return hi, (x - hi.astype(F32)).astype(BF16)


def tall(x):
    hi, lo = halves(x)
    return jnp.concatenate([hi, lo, hi], axis=0)


def mm(w, x):
    return jnp.dot(w, tall(x), preferred_element_type=F32)


def loop(count, unroll, step):
    def several(i, carry):
        for u in range(unroll):
            step(i * unroll + u)
        return carry

    if unroll == count:
        several(0, 0)
    else:
        lax.fori_loop(0, count // unroll, several, 0)


def rows_at(at, size):
    return pl.ds(at if isinstance(at, int) else pl.multiple_of(at, 8), size)


def swap(a, b, low):
    return jnp.where(low, a, pltpu.roll(b, 64, 1)), jnp.where(low, pltpu.roll(a, 64, 1), b)


def absorb_kernel(env, p, ops, out, env_s, p_s, q_s, ops_s, x_s, t_s, s_s, bra_w, ket_w, env_sem, p_sem, ops_sem):
    def tensor(j):
        part = pl.ds(128 * j, 128)
        return pltpu.make_async_copy(p.at[part], p_s.at[part], p_sem.at[j])

    small = [tensor(0), pltpu.make_async_copy(ops, ops_s, ops_sem)]
    for copy in small:
        copy.start()

    def chunk(kl):
        rows = pl.ds(8 * kl, 8)
        return pltpu.make_async_copy(env.at[:, :, rows, :], env_s.at[:, :, rows, :], env_sem.at[kl])

    for kl in range(8):
        chunk(kl).start(priority=1)
    tensor(1).start(priority=1)
    low = lax.broadcasted_iota(jnp.int32, (8, 128), 1) < 64
    for copy in small:
        copy.wait()
    def weights(j):
        for g in range(16):
            part = pl.ds(64 * (g // 8) + g % 8, 8, stride=8) if j == 0 else pl.ds(128 + 8 * g, 8)
            q_s[:, 128 * j + 8 * g : 128 * j + 8 * g + 8, :] = jnp.swapaxes(p_s[part], 0, 1)
        w = jnp.concatenate([q_s[d, 128 * j : 128 * (j + 1), :].T for d in range(8)], axis=0)
        for a in range(2):
            hi, lo = halves(ops_s[j, a, 0] * w[:, :64] + ops_s[j, a, 1] * w[:, 64:])
            bra_w[j, 64 * a : 64 * (a + 1), :] = jnp.concatenate([hi, hi, lo], axis=1)
        hi, lo = halves(w)
        ket_w[j, :64] = jnp.concatenate([hi, hi], axis=1)
        ket_w[j, 64:] = jnp.concatenate([lo, jnp.zeros_like(lo)], axis=1)

    weights(0)
    if not LATE:
        weights(1)

    def first(kl, k0):
        rows = rows_at(8 * kl, 8)
        pieces = []
        for c in range(4):
            lanes = pl.ds(k0 * 512 + 128 * c, 128)
            pieces += swap(env_s[0, 0, rows, lanes], env_s[1, 0, rows, lanes], low)
        return jnp.concatenate(pieces, axis=0)

    def second(at):
        return x_s[rows_at(at * 64, 64), :]

    def bra_group(j, places, xs):
        y = mm(bra_w[j], jnp.concatenate(xs, axis=1))
        for g in range(G):
            for a in range(2):
                t_s[pl.ds(a * 64 + places[g], 64, stride=RS), :] = y[64 * a : 64 * (a + 1), 128 * g : 128 * (g + 1)]

    for start in range(0, 8, W0):
        for kl in range(start, start + W0):
            chunk(kl).wait()
        for kl in range(start, start + W0):
            for k0 in range(0, 8, G):
                bra_group(0, [(k0 + g) * 8 + kl for g in range(G)], [first(kl, k0 + g) for g in range(G)])

    def ket(j, br, put):
        for start in range(0, 8, G):
            x = jnp.concatenate([t_s[pl.ds(((start + g) * 8 + br) * RS, 128), :] for g in range(G)], axis=1)
            x = jnp.concatenate(halves(x), axis=0)
            if KM:
                y = jnp.dot(ket_w[j], x, preferred_element_type=F32)
                y = y[:64] + y[64:]
            else:
                y = jnp.dot(ket_w[j, :64], x, preferred_element_type=F32) + jnp.dot(ket_w[j, 64:], x, preferred_element_type=F32)
            for g in range(G):
                put((start + g) * 8 + br, y[:, 128 * g : 128 * (g + 1)])

    def put0(b, y):
        bd, br = b // 8, b % 8
        for kd in range(8):
            s_s[pl.ds(br * 8 * BS + (bd % 2) * 32 + kd * 4 + bd // 2, 8, stride=BS), :] = y[8 * kd : 8 * (kd + 1)]

    def turned(i):
        return jnp.concatenate([s_s[pl.ds(2 * i * BS, 64), :], s_s[pl.ds((2 * i + 1) * BS, 64), :]], axis=0).T

    def sweep(j, put, finish):
        def step(br):
            ket(j, br, put)
            for i in range(4):
                finish(br * 4 + i)

        loop(8, UBR, step)

    def turn(i):
        br, kr = i // 4, 2 * (i % 4)
        z = turned(i)
        for k1 in range(8):
            z0, z1 = swap(z[8 * k1 : 8 * k1 + 8], z[64 + 8 * k1 : 64 + 8 * k1 + 8], low)
            x_s[rows_at((kr * 8 + k1) * 64 + br * 8, 8), :] = z0
            x_s[rows_at((kr * 8 + 8 + k1) * 64 + br * 8, 8), :] = z1

    if LATE:
        tensor(1).wait()
        weights(1)
    sweep(0, put0, turn)
    loop(64 // G, UB, lambda i: bra_group(1, [i * G + g for g in range(G)], [second(i * G + g) for g in range(G)]))

    def put1(b, y):
        bd, br = b // 8, b % 8
        for kd in range(8):
            s_s[pl.ds(kd * 8 + bd + br * 8 * BS, 8, stride=BS), :] = y[8 * kd : 8 * (kd + 1)]

    def leave(i):
        br, kr = i // 4, 2 * (i % 4)
        z = turned(i)
        for e in range(2):
            for r in range(4):
                z0, z1 = swap(z[64 * e + 8 * r : 64 * e + 8 * r + 8], z[64 * e + 32 + 8 * r : 64 * e + 40 + 8 * r], low)
                h, row = r // 2, 16 * e + 8 * (r % 2)
                out[2 * (kr * 8 + br) + h, row : row + 8, :] = z0
                out[2 * (kr * 8 + 8 + br) + h, row : row + 8, :] = z1

    sweep(1, put1, leave)


HBM = pl.BlockSpec(memory_space=pltpu.HBM)
VMEM = pl.BlockSpec(memory_space=pltpu.VMEM)


def absorb(env, p, ops):
    return pl.pallas_call(
        absorb_kernel,
        out_shape=jax.ShapeDtypeStruct((128, 32, 128), F32),
        in_specs=[HBM, HBM, HBM],
        out_specs=VMEM,
        scratch_shapes=[
            pltpu.VMEM((2, 1, 64, 4096), F32),
            pltpu.VMEM((256, 8, 8), F32),
            pltpu.VMEM((8, 256, 8), F32),
            pltpu.SMEM((2, 2, 2), F32),
            pltpu.VMEM((4096, 128), F32),
            pltpu.VMEM((64 * RS, 128), F32),
            pltpu.VMEM((64 * BS, 128), F32),
            pltpu.VMEM((2, 128, 192), BF16),
            pltpu.VMEM((2, 128, 256), BF16),
            pltpu.SemaphoreType.DMA((8,)),
            pltpu.SemaphoreType.DMA((2,)),
            pltpu.SemaphoreType.DMA,
        ],
        compiler_params=pltpu.CompilerParams(vmem_limit_bytes=40 << 20),
        cost_estimate=pl.CostEstimate(flops=2 << 30, bytes_accessed=4 << 20, transcendentals=0),
        name="absorb",
    )(env, p, ops)


def absorb_raw(env, peps, ops):
    return absorb(*[pltpu.with_memory_space_constraint(v, pltpu.HBM) for v in (env, peps.reshape(256, 8, 8), ops)])


def gauge_kernel(r, gm, out, sq, w_s, x_s):
    hi, lo = halves(gm[...])
    w_s[:128] = jnp.concatenate([hi, hi], axis=1)
    w_s[128:] = jnp.concatenate([lo, jnp.zeros_like(lo)], axis=1)
    low = lax.broadcasted_iota(jnp.int32, (1, 128), 1) < 64
    sums = []
    for e in range(2):
        tot = jnp.zeros((8, 128), F32)
        for t in (2 * e, 2 * e + 1):
            for m in range(16):
                part = jnp.swapaxes(r[8 * m : 8 * m + 8, 8 * t : 8 * t + 8, :], 0, 1)
                for s in range(8):
                    x_s[8 * t + s, 8 * m : 8 * m + 8, :] = part[s]
            for b in range(8 * t, 8 * t + 8, 4):
                x = jnp.concatenate([x_s[b + g] for g in range(4)], axis=1)
                y = jnp.dot(w_s[...], jnp.concatenate(halves(x), axis=0), preferred_element_type=F32)
                y = y[:128] + y[128:]
                out[e, :, 128 * (b - 16 * e) : 128 * (b - 16 * e + 4)] = y
                q = (y * y).reshape(16, 8, 128 * 4).sum(0)
                for g in range(4):
                    tot = tot + q[:, 128 * g : 128 * (g + 1)]
        part = jnp.sum(tot, axis=0, keepdims=True)
        sums.append(part + pltpu.roll(part, 64, 1))
    sq[...] = jnp.broadcast_to(jnp.where(low, sums[0], sums[1]), (128, 128))


def gauge(r, gm):
    return pl.pallas_call(
        gauge_kernel,
        out_shape=(jax.ShapeDtypeStruct((2, 128, 2048), F32), jax.ShapeDtypeStruct((128, 128), F32)),
        in_specs=[VMEM, VMEM],
        out_specs=(VMEM, VMEM),
        scratch_shapes=[pltpu.VMEM((256, 256), BF16), pltpu.VMEM((32, 128, 128), F32)],
        compiler_params=pltpu.CompilerParams(vmem_limit_bytes=40 << 20),
        cost_estimate=pl.CostEstimate(flops=1 << 29, bytes_accessed=4 << 20, transcendentals=0),
        name="gauge",
    )(r, gm)


def scale_kernel(entries, x, sums, out, rms, y_s, rms_s, sems, rms_sem):
    total = jnp.sum(sums[...], axis=0, keepdims=True)
    low = lax.broadcasted_iota(jnp.int32, (1, 128), 1) < 64
    copies = []
    means = [jnp.sum(jnp.where(half, total, 0.0), axis=1, keepdims=True) / entries for half in (low, ~low)]
    for e in range(2):
        factor = lax.rsqrt(means[e] + EPS)
        for c in range(4):
            at = pl.ds(128 // 4 * c, 128 // 4)
            y_s[e, at, :] = x[e, at, :] * factor
            copy = pltpu.make_async_copy(y_s.at[e, at, :], out.at[e, at, :], sems.at[4 * e + c])
            copy.start()
            copies.append(copy)
    for e in range(2):
        rms_s[e] = jnp.sqrt(means[e])[0, 0]
    copy = pltpu.make_async_copy(rms_s, rms, rms_sem)
    copy.start()
    copies.append(copy)
    for copy in copies:
        copy.wait()


def scale(x, sums, entries):
    return pl.pallas_call(
        functools.partial(scale_kernel, entries),
        out_shape=(jax.ShapeDtypeStruct((2, 128, 2048), F32), jax.ShapeDtypeStruct((2,), F32)),
        in_specs=[VMEM, VMEM],
        out_specs=(HBM, HBM),
        scratch_shapes=[
            pltpu.VMEM((2, 128, 2048), F32),
            pltpu.SMEM((2,), F32),
            pltpu.SemaphoreType.DMA((2 * 4,)),
            pltpu.SemaphoreType.DMA,
        ],
        compiler_params=pltpu.CompilerParams(vmem_limit_bytes=40 << 20),
        cost_estimate=pl.CostEstimate(flops=1 << 19, bytes_accessed=4 << 20, transcendentals=0),
        name="scale",
    )(x, sums)


def body(environment, peps, operators, gauge_matrix):
    blocks = absorb_raw(environment, peps, operators)
    merged = lax.all_to_all(blocks, BITS, 0, 0, tiled=True)
    gauged, sums = gauge(merged, gauge_matrix)
    sums = lax.all_to_all(sums, BITS, 0, 0, tiled=True)
    entries = gauged.shape[1] * gauged.shape[2] * lax.axis_size(BITS)
    return scale(gauged, sums, entries)


def solution(mesh):
    torus = Mesh(mesh.devices.reshape(4, 4, 4, 2), BITS)
    in_specs = (P(None, BITS, None, None), P(), P(), P())
    out_specs = (P(None, None, BITS), P())
    return jax.shard_map(body, mesh=torus, in_specs=in_specs, out_specs=out_specs, check_vma=False)
```
